32 devices in a mesh: tm: 8 (over z, y), freq: 4 (over x, core).
Axes of the slice: x: 2, y: 2, z: 4, core: 2. Of those that a mesh axis runs over, the one named last changes fastest.
Arguments:
- visibilities: bfloat16 [2, 64, 1024, 1024], P(None, 'freq', 'tm'), may hold values from -6 to 6
- projection: bfloat16 [16, 64, 2, 2, 64, 512], P('tm', 'freq'), may hold values from -0.1875 to 0.1875
- kl_weight: bfloat16 [16, 2, 64, 64], P('tm'), may hold values from -0.5 to 0.5
- azimuthal: int32 [16], replicated, may hold values from 0 to 1023, as said below
- live_mode_totals: int32 [16, 64, 2], P('tm', 'freq'), may hold values from 1 to 64, as said below
Outputs:
- kl_modes: float32 [16, 2, 64, 2, 64], P('tm', None, None, None, 'freq')
The draws below stay inside these ranges and needn't reach their ends.
Inputs may be any that keep to these rules, and one draw needn't show every extreme that they name: `azimuthal`: the m values are distinct. `live_mode_totals`: slots from the count up to 64 are padding; the count 64 occurs in every draw.
All inputs are finite; a program needn't handle non-finite values.
Results may differ from the reference program's by a relative error of at most 0.012.
Values may be sent and summed in bfloat16 or wider, within the bound.
A program may use at most 192 MiB of HBM per device.

```python
import math
import jax
import jax.numpy as jnp
from jax import lax

BL = 512
POL = 2
F = 64
TIMES = 1024
MODES = 64
M = 16


def draw_azimuthal(key, part):
    return jax.random.permutation(key, TIMES)[:M].astype(jnp.int32)


def draw_live_mode_totals(key, part):
    counts = jax.random.randint(key, (M * F * POL,), 1, MODES + 1, dtype=jnp.int32)
    where_full = jax.random.randint(jax.random.fold_in(key, 7), (), 0, M * F * POL, dtype=jnp.int32)
    counts = counts.at[where_full].set(MODES)
    return counts.reshape(M, F, POL)


def levels(stream_key, extent, shards, low, top_value):
    def one(position, shards_of):
        heights = jax.random.uniform(jax.random.fold_in(jax.random.fold_in(stream_key, 6), position), (shards_of,), jnp.float32, low / len(shards), top_value / len(shards))
        return jnp.repeat(jnp.exp(heights), extent[position] // shards_of).reshape((-1,) + (1,) * (len(extent) - position - 1))

    level = one(*shards[0])
    for cut in shards[1:]:
        level = level * one(*cut)
    return level


def gaussian(stream_key, shape, deviation, reach, pieces=(), held_as=jnp.bfloat16):
    entries = jax.random.normal(stream_key, shape, jnp.float32) * deviation
    if len(pieces) > 0:
        entries = levels(stream_key, shape, pieces, -0.22, 0.18) * entries
    return jnp.clip(entries, min=-reach, max=reach).astype(held_as)


def setup_inputs(seed: int = 0) -> dict:
    key_of = jax.random.split(jax.random.key(seed), 6)
    return {
        "visibilities": gaussian(key_of[0], (2, F, TIMES, POL * BL), 1.0, 6.0, ((1, 4), (2, 8))),
        "projection": gaussian(key_of[1], (M, F, POL, 2, MODES, BL), (2 * BL) ** -0.5, 0.1875, ((0, 8), (1, 4))),
        "kl_weight": gaussian(key_of[2], (M, 2, F, F), (2 * F) ** -0.5, 0.5, ((0, 8),)),
        "azimuthal": draw_azimuthal(jax.random.fold_in(key_of[5], 71), 0),
        "live_mode_totals": draw_live_mode_totals(jax.random.fold_in(key_of[5], 71), 0),
    }


def reference(visibilities, projection, kl_weight, azimuthal, live_mode_totals):
    time_index = jnp.arange(TIMES, dtype=jnp.int32)
    phase_index = azimuthal.astype(jnp.int32)[:, None] * time_index[None, :] % TIMES
    angles = phase_index.astype(jnp.float32) * (2.0 * math.pi / TIMES)
    cosine_table = jnp.cos(angles)
    sine_table = jnp.sin(angles)
    norm_factor = 1.0 / math.sqrt(TIMES)
    highest = lax.Precision.HIGHEST

    def per_channel(channel):
        real_part = visibilities[0, channel].astype(jnp.float32)
        imag_part = visibilities[1, channel].astype(jnp.float32)
        out_real = jnp.dot(cosine_table, real_part, precision=highest) + jnp.dot(sine_table, imag_part, precision=highest)
        out_imag = jnp.dot(cosine_table, imag_part, precision=highest) - jnp.dot(sine_table, real_part, precision=highest)
        return jnp.stack([out_real, out_imag], axis=1) * norm_factor
    mode_spectra = lax.map(per_channel, jnp.arange(F, dtype=jnp.int32))
    mode_spectra = jnp.transpose(mode_spectra, (1, 0, 2, 3)).astype(jnp.bfloat16)
    mode_spectra = mode_spectra.reshape(M, F, 2, POL, BL)
    modes_iota = jnp.arange(MODES, dtype=jnp.int32)

    def slot_entries(inputs):
        matrix, vector, counts = inputs
        matrix_f = matrix.astype(jnp.float32)
        vector_f = vector.astype(jnp.float32)

        def apply_map(mat_part, vec_part):
            return jnp.einsum('fpkb,fpb->fpk', mat_part, vec_part)
        proj_real = apply_map(matrix_f[:, :, 0], vector_f[:, 0]) - apply_map(matrix_f[:, :, 1], vector_f[:, 1])
        proj_imag = apply_map(matrix_f[:, :, 0], vector_f[:, 1]) + apply_map(matrix_f[:, :, 1], vector_f[:, 0])
        live_slots = modes_iota[None, None, :] < counts[:, :, None]
        stacked_modes = jnp.stack([proj_real, proj_imag], axis=1)
        return jnp.where(live_slots[:, None], stacked_modes, 0.0).astype(jnp.bfloat16)
    projected = lax.map(slot_entries, (projection, mode_spectra, live_mode_totals))
    weights = kl_weight.astype(jnp.float32)
    values = projected.astype(jnp.float32)

    def kl_mix(weight_part, value_part):
        return jnp.einsum('sgc,scpk->sgpk', weight_part, value_part)
    mixed_real = kl_mix(weights[:, 0], values[:, :, 0]) - kl_mix(weights[:, 1], values[:, :, 1])
    mixed_imag = kl_mix(weights[:, 0], values[:, :, 1]) + kl_mix(weights[:, 1], values[:, :, 0])
    return jnp.stack([mixed_real, mixed_imag], axis=1)
```

```python
import functools
import math

import jax
import jax.numpy as jnp
from jax import lax
from jax.experimental import pallas as pl
from jax.experimental.pallas import tpu as pltpu
from jax.sharding import PartitionSpec as P

MESH = pl.DeviceIdType.MESH
INNER = 2
CB = 2
LAG = 3


def sin_half(x):
    y = x * x
    acc = jnp.full_like(x, -1.0 / math.factorial(15))
    for n in (13, 11, 9, 7, 5, 3, 1):
        sign = 1.0 if n % 4 == 1 else -1.0
        acc = acc * y + sign / math.factorial(n)
    return acc * x


def build_tables(az_ref, m_total, nz, slots, time_dev, time_total, time_base):
    rows, depth = nz * INNER * slots * 4, 2 * time_dev
    row = lax.broadcasted_iota(jnp.int32, (rows, depth), 0)
    col = lax.broadcasted_iota(jnp.int32, (rows, depth), 1)
    q = row % 2
    s = (row // 2) % slots
    half = (row // (2 * slots)) % 2
    dest = row // (4 * slots)
    inner, outer = dest // nz, dest % nz
    m_index = (outer * INNER + inner) * slots + s
    order = jnp.zeros((rows, depth), jnp.int32)
    for m in range(m_total):
        order = jnp.where(m_index == m, az_ref[m], order)
    part = col // time_dev
    t = time_base + col % time_dev
    quarter = time_total // 4
    shift = jnp.where(q == part, 0, jnp.where(q == 0, -quarter, quarter))
    phase = (order * t + shift) & (time_total - 1)
    phase = jnp.where(phase > time_total // 2, phase - time_total, phase)
    sn = sin_half(phase.astype(jnp.float32) * (math.pi / time_total))
    value = (1.0 - 2.0 * sn * sn) * (1.0 / math.sqrt(time_total))
    upper = value.astype(jnp.bfloat16)
    lower = (value - upper.astype(jnp.float32)).astype(jnp.bfloat16)
    return jnp.where(half == 0, upper.astype(jnp.float32), lower.astype(jnp.float32)).astype(jnp.bfloat16)


def kernel(
    dims, az_hbm, live_hbm, vis_ref, proj_ref, kl_hbm, out_ref,
    vbuf, pbuf, az_ref, live_ref, kl_ref, table, sbuf, rbuf1, sbuf2, rbuf2, rlast, keep, pall, lhs, res,
    vsem, psem, csem, ysend, yrecv, zsend, zrecv, fsend, frecv,
):
    nz, nf, units, slots, pols, bl, modes, chans, time_dev, time_total, m_total = dims
    tm, fi = lax.axis_index("tm"), lax.axis_index("freq")
    zi, yi = tm // INNER, tm % INNER
    partner = zi * INNER + (1 - yi)
    last = units - 1

    def z_peer(o):
        return lax.rem(zi + o, nz) * INNER + yi

    def f_peer(o):
        return lax.rem(fi + o, nf)

    def vis_copy(u, part):
        return pltpu.make_async_copy(
            vis_ref.at[part, pl.ds(u * CB, CB)],
            vbuf.at[u, :, pl.ds(part * time_dev, time_dev), :],
            vsem.at[u, part],
        )

    def proj_copy(u):
        return pltpu.make_async_copy(proj_ref.at[:, pl.ds(u * CB, CB)], pbuf.at[u], psem.at[u])

    def y_copy(u):
        return pltpu.make_async_remote_copy(
            src_ref=sbuf.at[u, 1 - yi], dst_ref=rbuf1.at[u],
            send_sem=ysend.at[u], recv_sem=yrecv.at[u],
            device_id=(partner, fi), device_id_type=MESH,
        )

    def y_last():
        return pltpu.make_async_remote_copy(
            src_ref=sbuf2.at[last, 0], dst_ref=rbuf1.at[last, 0],
            send_sem=ysend.at[last], recv_sem=yrecv.at[last],
            device_id=(partner, fi), device_id_type=MESH,
        )

    def z_copy(u, o):
        return pltpu.make_async_remote_copy(
            src_ref=sbuf2.at[u, lax.rem(zi + o, nz)], dst_ref=rbuf2.at[u, o - 1],
            send_sem=zsend.at[u, o - 1], recv_sem=zrecv.at[u, o - 1],
            device_id=(z_peer(o), fi), device_id_type=MESH,
        )

    def z_last(o):
        return pltpu.make_async_remote_copy(
            src_ref=sbuf.at[last, :, lax.rem(zi + o, nz)], dst_ref=rlast.at[o - 1],
            send_sem=zsend.at[last, o - 1], recv_sem=zrecv.at[last, o - 1],
            device_id=(z_peer(o), fi), device_id_type=MESH,
        )

    def f_copy(u, o):
        return pltpu.make_async_remote_copy(
            src_ref=pall.at[fi, u], dst_ref=pall.at[fi, u],
            send_sem=fsend.at[u, o - 1], recv_sem=frecv.at[u, o - 1],
            device_id=(tm, f_peer(o)), device_id_type=MESH,
        )

    def f_arrival(u, o):
        source = lax.rem(fi + nf - o, nf)
        return pltpu.make_async_remote_copy(
            src_ref=pall.at[source, u], dst_ref=pall.at[source, u],
            send_sem=fsend.at[u, o - 1], recv_sem=frecv.at[u, o - 1],
            device_id=(tm, f_peer(o)), device_id_type=MESH,
        )

    az_copy = pltpu.make_async_copy(az_hbm, az_ref, csem.at[0])
    live_copy = pltpu.make_async_copy(live_hbm, live_ref, csem.at[1])
    kl_copy = pltpu.make_async_copy(kl_hbm, kl_ref, csem.at[2])

    az_copy.start()
    barrier = pltpu.get_barrier_semaphore()
    pl.semaphore_signal(barrier, inc=1, device_id=(partner, fi), device_id_type=MESH)
    for o in range(1, nz):
        pl.semaphore_signal(barrier, inc=1, device_id=(z_peer(o), fi), device_id_type=MESH)
    for o in range(1, nf):
        pl.semaphore_signal(barrier, inc=1, device_id=(tm, f_peer(o)), device_id_type=MESH)
    for u in (0, last, *range(1, last)):
        for part in range(2):
            vis_copy(u, part).start()
    live_copy.start()
    kl_copy.start()

    az_copy.wait()
    table[...] = build_tables(az_ref, m_total, nz, slots, time_dev, time_total, tm * time_dev)

    dests = nz * INNER
    rows = 4 * CB
    cols = pols * bl
    sub = lax.broadcasted_iota(jnp.int32, (dests, rows, cols), 1)

    def transform(u):
        for part in range(2):
            vis_copy(u, part).wait()
        pair = []
        for c in range(CB):
            x = jnp.dot(table[...], vbuf[u, c], preferred_element_type=jnp.float32)
            x = x.reshape(dests, rows, cols)
            pair.append(x + pltpu.roll(x, 4, 1))
        block = jnp.where(sub < 4, pair[0], pair[1]).astype(jnp.bfloat16)
        sbuf[u] = block.reshape(INNER, nz, rows, cols)

    transform(0)
    pl.semaphore_wait(barrier, nz + nf - 1)
    y_copy(0).start()
    transform(last)
    for o in range(1, nz):
        z_last(o).start()

    def spread_units(u, carry):
        transform(u)
        y_copy(u).start()
        return carry

    lax.fori_loop(1, last, spread_units, 0)
    for u in range(units):
        proj_copy(u).start()

    kl_copy.wait()
    live_copy.wait()
    width = chans * slots * 2
    spread_row = lax.broadcasted_iota(jnp.int32, (chans, width), 0)
    spread_col = lax.broadcasted_iota(jnp.int32, (chans, width), 1)
    spread = jnp.where(spread_col // (slots * 2) == spread_row, 1.0, 0.0).astype(jnp.bfloat16)
    lane = lax.broadcasted_iota(jnp.int32, (chans, width), 1) % (slots * 2)
    for s in range(slots):
        w_re = jnp.dot(kl_ref[s, 0], spread, preferred_element_type=jnp.float32)
        w_im = jnp.dot(kl_ref[s, 1], spread, preferred_element_type=jnp.float32)
        lhs[s, 0] = jnp.where(lane == 2 * s, w_re, jnp.where(lane == 2 * s + 1, -w_im, 0.0)).astype(jnp.bfloat16)
        lhs[s, 1] = jnp.where(lane == 2 * s, w_im, jnp.where(lane == 2 * s + 1, w_re, 0.0)).astype(jnp.bfloat16)

    prow = lax.broadcasted_iota(jnp.int32, (rows, 2 * modes), 0)
    plane = lax.broadcasted_iota(jnp.int32, (rows, 2 * modes), 1)

    def combine(u):
        y_copy(u).wait_recv()
        sbuf2[u] = (sbuf[u, yi].astype(jnp.float32) + rbuf1[u].astype(jnp.float32)).astype(jnp.bfloat16)
        for o in range(1, nz):
            z_copy(u, o).start()

    def combine_last():
        total = sbuf[last, :, zi].astype(jnp.float32)
        for o in range(1, nz):
            z_last(o).wait_recv()
            total = total + rlast[o - 1].astype(jnp.float32)
        mine = yi == 0
        keep[...] = jnp.where(mine, total[0], total[1])
        sbuf2[last, 0] = jnp.where(mine, total[1], total[0]).astype(jnp.bfloat16)
        y_last().start()

    def project(u, total):
        proj_copy(u).wait()
        vectors = jnp.concatenate([total[:, p * bl:(p + 1) * bl] for p in range(pols)], axis=0).astype(jnp.bfloat16)
        first = jnp.zeros((rows, 2 * modes), jnp.float32)
        second = first
        count = jnp.zeros((rows, 2 * modes), jnp.int32)
        for c in range(CB):
            for s in range(slots):
                part = lax.dot_general(
                    vectors, pbuf[u, s, c], (((1,), (1,)), ((), ())), preferred_element_type=jnp.float32
                )
                here = prow // 2 == c * slots + s
                first = jnp.where(here, part[:rows, :2 * modes], first)
                second = jnp.where(here, part[rows:, 2 * modes:], second)
                live = [live_ref[s, p, u * CB + c] for p in range(pols)]
                count = jnp.where(here, jnp.where(plane < modes, live[0], live[1]), count)
        low = plane < modes
        direct = jnp.where(low, first, pltpu.roll(second, modes, 1))
        cross = jnp.where(low, pltpu.roll(first, modes, 1), second)
        real_row = prow % 2 == 0
        cross = jnp.where(real_row, -pltpu.roll(cross, rows - 1, 0), pltpu.roll(cross, 1, 0))
        kept = jnp.where(plane % modes < count, direct + cross, 0.0)
        pall[fi, u] = kept.astype(jnp.bfloat16)
        for o in range(1, nf):
            f_copy(u, o).start()

    def project_outer(u):
        total = sbuf2[u, zi].astype(jnp.float32)
        for o in range(1, nz):
            z_copy(u, o).wait_recv()
            total = total + rbuf2[u, o - 1].astype(jnp.float32)
        project(u, total)

    def project_last():
        y_last().wait_recv()
        project(last, keep[...] + rbuf1[last, 0].astype(jnp.float32))

    def step(u, carry):
        @pl.when(u < last)
        def _():
            combine(u)

        @pl.when(u == last - LAG)
        def _():
            combine_last()

        @pl.when(u >= LAG)
        def _():
            project_outer(u - LAG)

        @pl.when(u == last)
        def _():
            project_last()

        return carry

    lax.fori_loop(0, last + LAG, step, 0)

    def drain(u, carry):
        y_copy(u).wait_send()
        for o in range(1, nz):
            z_copy(u, o).wait_send()
        return carry

    lax.fori_loop(0, last, drain, 0)
    y_last().wait_send()
    for o in range(1, nz):
        z_last(o).wait_send()

    def arrivals(u, carry):
        for o in range(1, nf):
            f_copy(u, o).wait_send()
            f_arrival(u, o).wait_recv()
        return carry

    lax.fori_loop(0, units, arrivals, 0)

    gathered = pall[...].reshape(nf * units * rows, 2 * modes)
    per = modes // nf
    for s in range(slots):
        for q in range(2):
            i = 2 * s + q
            res[i] = lax.dot_general(
                gathered, lhs[s, q], (((0,), (1,)), ((), ())), preferred_element_type=jnp.float32
            )
            for p in range(pols):
                at = pl.multiple_of(p * modes + fi * per, per)
                out_ref[s, q, p] = res[i, pl.ds(at, per), :]


def shards(visibilities, projection, kl_weight, azimuthal, live_mode_totals):
    nt, nf = lax.axis_size("tm"), lax.axis_size("freq")
    nz = nt // INNER
    time_dev, columns = visibilities.shape[2], visibilities.shape[3]
    slots, per_dev, pols, _, modes, bl = projection.shape
    chans = kl_weight.shape[3]
    units = per_dev // CB
    time_total = time_dev * nt
    m_total = azimuthal.shape[0]
    assert slots == 2 and pols == 2 and time_total & (time_total - 1) == 0 and units > LAG + 1
    rows = 4 * CB
    dims = (nz, nf, units, slots, pols, bl, modes, chans, time_dev, time_total, m_total)
    bf16, f32 = jnp.bfloat16, jnp.float32
    flat = projection.reshape(slots, per_dev, pols * 2 * modes, bl)
    live = jnp.swapaxes(live_mode_totals, 1, 2)
    out = pl.pallas_call(
        functools.partial(kernel, dims),
        out_shape=pltpu.VMEM((slots, 2, pols, modes // nf, chans), f32),
        in_specs=[pl.BlockSpec(memory_space=pl.ANY)] * 5,
        out_specs=pl.BlockSpec(memory_space=pltpu.VMEM),
        scratch_shapes=[
            pltpu.VMEM((units, CB, 2 * time_dev, columns), bf16),
            pltpu.VMEM((units, slots, CB, pols * 2 * modes, bl), bf16),
            pltpu.SMEM(azimuthal.shape, jnp.int32),
            pltpu.SMEM(live.shape, jnp.int32),
            pltpu.VMEM(kl_weight.shape, bf16),
            pltpu.VMEM((nt * 8, 2 * time_dev), bf16),
            pltpu.VMEM((units, INNER, nz, rows, columns), bf16),
            pltpu.VMEM((units, nz, rows, columns), bf16),
            pltpu.VMEM((units, nz, rows, columns), bf16),
            pltpu.VMEM((units, nz - 1, rows, columns), bf16),
            pltpu.VMEM((nz - 1, INNER, rows, columns), bf16),
            pltpu.VMEM((rows, columns), f32),
            pltpu.VMEM((nf, units, rows, 2 * modes), bf16),
            pltpu.VMEM((slots, 2, chans, chans * slots * 2), bf16),
            pltpu.VMEM((slots * 2, pols * modes, chans), f32),
            pltpu.SemaphoreType.DMA((units, 2)),
            pltpu.SemaphoreType.DMA((units,)),
            pltpu.SemaphoreType.DMA((3,)),
            pltpu.SemaphoreType.DMA((units,)),
            pltpu.SemaphoreType.DMA((units,)),
            pltpu.SemaphoreType.DMA((units, nz - 1)),
            pltpu.SemaphoreType.DMA((units, nz - 1)),
            pltpu.SemaphoreType.DMA((units, nf - 1)),
            pltpu.SemaphoreType.DMA((units, nf - 1)),
        ],
        compiler_params=pltpu.CompilerParams(collective_id=0, has_side_effects=True),
    )(azimuthal, live, visibilities, flat, kl_weight)
    return jnp.transpose(out, (0, 1, 4, 2, 3))


def solution(mesh):
    return jax.shard_map(
        shards,
        mesh=mesh,
        in_specs=(
            P(None, "freq", "tm", None),
            P("tm", "freq", None, None, None, None),
            P("tm", None, None, None),
            P(),
            P("tm", "freq", None),
        ),
        out_specs=P("tm", None, None, None, "freq"),
        check_vma=False,
    )
```

```python
import functools
import math

import jax
import jax.numpy as jnp
from jax import lax
from jax.experimental import pallas as pl
from jax.experimental.pallas import tpu as pltpu
from jax.sharding import PartitionSpec as P

MESH = pl.DeviceIdType.MESH
INNER = 2
CB = 2
LAG = 3
LEAD = 2


def sin_half(x):
    y = x * x
    acc = jnp.full_like(x, -1.0 / math.factorial(15))
    for n in (13, 11, 9, 7, 5, 3, 1):
        sign = 1.0 if n % 4 == 1 else -1.0
        acc = acc * y + sign / math.factorial(n)
    return acc * x


def build_tables(az_ref, m_total, nz, slots, time_dev, time_total, time_base):
    rows, depth = nz * INNER * slots * 4, 2 * time_dev
    row = lax.broadcasted_iota(jnp.int32, (rows, depth), 0)
    col = lax.broadcasted_iota(jnp.int32, (rows, depth), 1)
    q = row % 2
    s = (row // 2) % slots
    half = (row // (2 * slots)) % 2
    dest = row // (4 * slots)
    inner, outer = dest // nz, dest % nz
    m_index = (outer * INNER + inner) * slots + s
    order = jnp.zeros((rows, depth), jnp.int32)
    for m in range(m_total):
        order = jnp.where(m_index == m, az_ref[m], order)
    part = col // time_dev
    t = time_base + col % time_dev
    quarter = time_total // 4
    shift = jnp.where(q == part, 0, jnp.where(q == 0, -quarter, quarter))
    phase = (order * t + shift) & (time_total - 1)
    phase = jnp.where(phase > time_total // 2, phase - time_total, phase)
    sn = sin_half(phase.astype(jnp.float32) * (math.pi / time_total))
    value = (1.0 - 2.0 * sn * sn) * (1.0 / math.sqrt(time_total))
    upper = value.astype(jnp.bfloat16)
    lower = (value - upper.astype(jnp.float32)).astype(jnp.bfloat16)
    return jnp.where(half == 0, upper.astype(jnp.float32), lower.astype(jnp.float32)).astype(jnp.bfloat16)


def kernel(
    dims, az_hbm, live_hbm, vis_ref, proj_ref, kl_hbm, out_ref,
    vbuf, pbuf, az_ref, live_ref, kl_ref, table, sbuf, rbuf1, sbuf2, rbuf2, rlast, keep, pall, lhs, res,
    vsem, psem, csem, ysend, yrecv, yrest, zsend, zrecv, fsend, frecv,
):
    nz, nf, units, slots, pols, bl, modes, chans, time_dev, time_total, m_total = dims
    tm, fi = lax.axis_index("tm"), lax.axis_index("freq")
    zi, yi = tm // INNER, tm % INNER
    partner = zi * INNER + (1 - yi)
    last = units - 1

    def z_peer(o):
        return lax.rem(zi + o, nz) * INNER + yi

    def f_peer(o):
        return lax.rem(fi + o, nf)

    def vis_copy(u):
        return pltpu.make_async_copy(vis_ref.at[:, pl.ds(u * CB, CB)], vbuf.at[u], vsem.at[u])

    def remote(src, dst, send, recv, device):
        return pltpu.make_async_remote_copy(
            src_ref=src, dst_ref=dst, send_sem=send, recv_sem=recv, device_id=device, device_id_type=MESH
        )

    def y_first(u):
        return remote(sbuf.at[u, 1 - yi, 0], rbuf1.at[u, 0], ysend.at[0], yrecv.at[u], (partner, fi))

    def y_rest(u):
        others = pl.ds(1, nz - 1)
        return remote(sbuf.at[u, 1 - yi, others], rbuf1.at[u, others], ysend.at[0], yrest.at[u], (partner, fi))

    def y_last():
        return remote(sbuf2.at[last, 0], rbuf1.at[last, 0], ysend.at[1], yrecv.at[last], (partner, fi))

    def z_copy(u, o):
        return remote(
            sbuf2.at[u, lax.rem(zi + o, nz)], rbuf2.at[u, o - 1], zsend.at[0], zrecv.at[u], (z_peer(o), fi)
        )

    def z_last(o):
        return remote(
            sbuf.at[last, :, lax.rem(zi + o, nz)], rlast.at[o - 1], zsend.at[1], zrecv.at[last], (z_peer(o), fi)
        )

    def f_copy(u, o):
        return remote(pall.at[fi, u], pall.at[fi, u], fsend.at[0], frecv.at[0], (tm, f_peer(o)))

    az_copy = pltpu.make_async_copy(az_hbm, az_ref, csem.at[0])
    live_copy = pltpu.make_async_copy(live_hbm, live_ref, csem.at[1])
    kl_copy = pltpu.make_async_copy(kl_hbm, kl_ref, csem.at[2])
    proj_copy = pltpu.make_async_copy(proj_ref, pbuf, psem.at[0])

    az_copy.start()
    barrier = pltpu.get_barrier_semaphore()
    pl.semaphore_signal(barrier, inc=1, device_id=(partner, fi), device_id_type=MESH)
    for o in range(1, nz):
        pl.semaphore_signal(barrier, inc=1, device_id=(z_peer(o), fi), device_id_type=MESH)
    for o in range(1, nf):
        pl.semaphore_signal(barrier, inc=1, device_id=(tm, f_peer(o)), device_id_type=MESH)
    for u in (0, last, *range(1, last)):
        vis_copy(u).start()
    live_copy.start()
    kl_copy.start()

    az_copy.wait()
    table[...] = build_tables(az_ref, m_total, nz, slots, time_dev, time_total, tm * time_dev)

    dests = nz * INNER
    rows = 4 * CB
    cols = pols * bl
    sub = lax.broadcasted_iota(jnp.int32, (dests, rows, cols), 1)

    def transform(u):
        vis_copy(u).wait()
        pair = []
        for c in range(CB):
            stream = jnp.concatenate([vbuf[u, 0, c], vbuf[u, 1, c]], axis=0)
            x = jnp.dot(table[...], stream, preferred_element_type=jnp.float32)
            x = x.reshape(dests, rows, cols)
            pair.append(x + pltpu.roll(x, 4, 1))
        block = jnp.where(sub < 4, pair[0], pair[1]).astype(jnp.bfloat16)
        sbuf[u] = block.reshape(INNER, nz, rows, cols)

    transform(0)
    pl.semaphore_wait(barrier, nz + nf - 1)
    y_first(0).start()
    y_rest(0).start()
    transform(last)
    for o in range(1, nz):
        z_last(o).start()

    def spread_units(u, carry):
        transform(u)
        y_first(u).start()

        @pl.when(u > LEAD)
        def _():
            y_rest(u - LEAD).start()

        return carry

    lax.fori_loop(1, last, spread_units, 0)
    proj_copy.start()

    kl_copy.wait()
    live_copy.wait()
    width = chans * slots * 2
    spread_row = lax.broadcasted_iota(jnp.int32, (chans, width), 0)
    spread_col = lax.broadcasted_iota(jnp.int32, (chans, width), 1)
    spread = jnp.where(spread_col // (slots * 2) == spread_row, 1.0, 0.0).astype(jnp.bfloat16)
    lane = lax.broadcasted_iota(jnp.int32, (chans, width), 1) % (slots * 2)
    for s in range(slots):
        w_re = jnp.dot(kl_ref[s, 0], spread, preferred_element_type=jnp.float32)
        w_im = jnp.dot(kl_ref[s, 1], spread, preferred_element_type=jnp.float32)
        lhs[s, 0] = jnp.where(lane == 2 * s, w_re, jnp.where(lane == 2 * s + 1, -w_im, 0.0)).astype(jnp.bfloat16)
        lhs[s, 1] = jnp.where(lane == 2 * s, w_im, jnp.where(lane == 2 * s + 1, w_re, 0.0)).astype(jnp.bfloat16)

    prow = lax.broadcasted_iota(jnp.int32, (rows, 2 * modes), 0)
    plane = lax.broadcasted_iota(jnp.int32, (rows, 2 * modes), 1)

    def combine_first(u):
        y_first(u).wait_recv()
        sbuf2[u, 0] = (sbuf[u, yi, 0].astype(jnp.float32) + rbuf1[u, 0].astype(jnp.float32)).astype(jnp.bfloat16)

        @pl.when(zi != 0)
        def _():
            z_copy(u, nz - zi).start()

    def combine_rest(u):
        y_rest(u).wait_recv()
        others = pl.ds(1, nz - 1)
        total = sbuf[u, yi, others].astype(jnp.float32) + rbuf1[u, others].astype(jnp.float32)
        sbuf2[u, others] = total.astype(jnp.bfloat16)
        for o in range(1, nz):
            @pl.when(zi + o != nz)
            def _():
                z_copy(u, o).start()

    def combine_last():
        remote(rlast, rlast, zsend.at[1], zrecv.at[last], (partner, fi)).wait_recv()
        total = sbuf[last, :, zi].astype(jnp.float32)
        for o in range(1, nz):
            total = total + rlast[o - 1].astype(jnp.float32)
        mine = yi == 0
        keep[...] = jnp.where(mine, total[0], total[1])
        sbuf2[last, 0] = jnp.where(mine, total[1], total[0]).astype(jnp.bfloat16)
        y_last().start()

    def project(u, total):
        vectors = jnp.concatenate([total[:, p * bl:(p + 1) * bl] for p in range(pols)], axis=0).astype(jnp.bfloat16)
        first = jnp.zeros((rows, 2 * modes), jnp.float32)
        second = first
        count = jnp.zeros((rows, 2 * modes), jnp.int32)
        for c in range(CB):
            for s in range(slots):
                part = lax.dot_general(
                    vectors, pbuf[s, u * CB + c], (((1,), (1,)), ((), ())), preferred_element_type=jnp.float32
                )
                here = prow // 2 == c * slots + s
                first = jnp.where(here, part[:rows, :2 * modes], first)
                second = jnp.where(here, part[rows:, 2 * modes:], second)
                live = [live_ref[s, p, u * CB + c] for p in range(pols)]
                count = jnp.where(here, jnp.where(plane < modes, live[0], live[1]), count)
        low = plane < modes
        direct = jnp.where(low, first, pltpu.roll(second, modes, 1))
        cross = jnp.where(low, pltpu.roll(first, modes, 1), second)
        real_row = prow % 2 == 0
        cross = jnp.where(real_row, -pltpu.roll(cross, rows - 1, 0), pltpu.roll(cross, 1, 0))
        kept = jnp.where(plane % modes < count, direct + cross, 0.0)
        pall[fi, u] = kept.astype(jnp.bfloat16)
        for o in range(1, nf):
            f_copy(u, o).start()

    def project_outer(u):
        remote(rbuf2.at[u], rbuf2.at[u], zsend.at[0], zrecv.at[u], (partner, fi)).wait_recv()
        total = sbuf2[u, zi].astype(jnp.float32)
        for o in range(1, nz):
            total = total + rbuf2[u, o - 1].astype(jnp.float32)
        project(u, total)

    def project_last():
        y_last().wait_recv()
        project(last, keep[...] + rbuf1[last, 0].astype(jnp.float32))

    lag = LAG + LEAD * jnp.minimum(zi, 1)

    def step(k, carry):
        @pl.when(k < last)
        def _():
            combine_first(k)

        @pl.when(k == 0)
        def _():
            combine_rest(0)

        @pl.when((k > LEAD) & (k < last + LEAD))
        def _():
            combine_rest(k - LEAD)

        @pl.when(k == LEAD)
        def _():
            proj_copy.wait()

        @pl.when(k == LEAD + 2)
        def _():
            combine_last()
            for u in range(last - LEAD, last):
                y_rest(u).start()

        @pl.when((k >= lag) & (k < last + lag))
        def _():
            project_outer(k - lag)

        @pl.when(k == last + 1)
        def _():
            project_last()

        return carry

    lax.fori_loop(0, last + LAG + LEAD, step, 0)

    everything = sbuf.at[pl.ds(0, last), 0]
    remote(everything, everything, ysend.at[0], yrecv.at[0], (partner, fi)).wait_send()
    y_last().wait_send()
    everything = sbuf2.at[pl.ds(0, last), pl.ds(0, nz - 1)]
    remote(everything, everything, zsend.at[0], zrecv.at[0], (partner, fi)).wait_send()
    remote(rlast, rlast, zsend.at[1], zrecv.at[last], (partner, fi)).wait_send()
    everything = pall.at[pl.ds(0, nf - 1)]
    gather = remote(everything, everything, fsend.at[0], frecv.at[0], (partner, fi))
    gather.wait_send()
    gather.wait_recv()

    gathered = pall[...].reshape(nf * units * rows, 2 * modes)
    per = modes // nf
    for s in range(slots):
        for q in range(2):
            i = 2 * s + q
            res[i] = lax.dot_general(
                gathered, lhs[s, q], (((0,), (1,)), ((), ())), preferred_element_type=jnp.float32
            )
            for p in range(pols):
                at = pl.multiple_of(p * modes + fi * per, per)
                out_ref[s, q, p] = res[i, pl.ds(at, per), :]


def shards(visibilities, projection, kl_weight, azimuthal, live_mode_totals):
    nt, nf = lax.axis_size("tm"), lax.axis_size("freq")
    nz = nt // INNER
    time_dev, columns = visibilities.shape[2], visibilities.shape[3]
    slots, per_dev, pols, _, modes, bl = projection.shape
    chans = kl_weight.shape[3]
    units = per_dev // CB
    time_total = time_dev * nt
    m_total = azimuthal.shape[0]
    assert slots == 2 and pols == 2 and time_total & (time_total - 1) == 0 and units > LEAD + 3
    rows = 4 * CB
    dims = (nz, nf, units, slots, pols, bl, modes, chans, time_dev, time_total, m_total)
    bf16, f32 = jnp.bfloat16, jnp.float32
    flat = projection.reshape(slots, per_dev, pols * 2 * modes, bl)
    live = jnp.swapaxes(live_mode_totals, 1, 2)
    out = pl.pallas_call(
        functools.partial(kernel, dims),
        out_shape=pltpu.VMEM((slots, 2, pols, modes // nf, chans), f32),
        in_specs=[pl.BlockSpec(memory_space=pl.ANY)] * 5,
        out_specs=pl.BlockSpec(memory_space=pltpu.VMEM),
        scratch_shapes=[
            pltpu.VMEM((units, 2, CB, time_dev, columns), bf16),
            pltpu.VMEM(flat.shape, bf16),
            pltpu.SMEM(azimuthal.shape, jnp.int32),
            pltpu.SMEM(live.shape, jnp.int32),
            pltpu.VMEM(kl_weight.shape, bf16),
            pltpu.VMEM((nt * 8, 2 * time_dev), bf16),
            pltpu.VMEM((units, INNER, nz, rows, columns), bf16),
            pltpu.VMEM((units, nz, rows, columns), bf16),
            pltpu.VMEM((units, nz, rows, columns), bf16),
            pltpu.VMEM((units, nz - 1, rows, columns), bf16),
            pltpu.VMEM((nz - 1, INNER, rows, columns), bf16),
            pltpu.VMEM((rows, columns), f32),
            pltpu.VMEM((nf, units, rows, 2 * modes), bf16),
            pltpu.VMEM((slots, 2, chans, chans * slots * 2), bf16),
            pltpu.VMEM((slots * 2, pols * modes, chans), f32),
            pltpu.SemaphoreType.DMA((units,)),
            pltpu.SemaphoreType.DMA((1,)),
            pltpu.SemaphoreType.DMA((3,)),
            pltpu.SemaphoreType.DMA((2,)),
            pltpu.SemaphoreType.DMA((units,)),
            pltpu.SemaphoreType.DMA((units - 1,)),
            pltpu.SemaphoreType.DMA((2,)),
            pltpu.SemaphoreType.DMA((units,)),
            pltpu.SemaphoreType.DMA((1,)),
            pltpu.SemaphoreType.DMA((1,)),
        ],
        compiler_params=pltpu.CompilerParams(collective_id=0, has_side_effects=True),
    )(azimuthal, live, visibilities, flat, kl_weight)
    return jnp.transpose(out, (0, 1, 4, 2, 3))


def solution(mesh):
    return jax.shard_map(
        shards,
        mesh=mesh,
        in_specs=(
            P(None, "freq", "tm", None),
            P("tm", "freq", None, None, None, None),
            P("tm", None, None, None),
            P(),
            P("tm", "freq", None),
        ),
        out_specs=P("tm", None, None, None, "freq"),
        check_vma=False,
    )
```

```python
import functools
import math

import jax
import jax.numpy as jnp
from jax import lax
from jax.experimental import pallas as pl
from jax.experimental.pallas import tpu as pltpu
from jax.sharding import PartitionSpec as P

MESH = pl.DeviceIdType.MESH
INNER = 2
CB = 2
DELAY = (0, 1, 2)
LAG = (5, 4, 4)


def sin_half(x):
    y = x * x
    acc = jnp.full_like(x, -1.0 / math.factorial(15))
    for n in (13, 11, 9, 7, 5, 3, 1):
        sign = 1.0 if n % 4 == 1 else -1.0
        acc = acc * y + sign / math.factorial(n)
    return acc * x


def place_of(z, nz):
    return jnp.where(z == 0, 0, jnp.where(z == nz - 1, 1, z + 1))


def build_tables(az_ref, m_total, nz, slots, time_dev, time_total, time_base):
    rows, depth = nz * INNER * slots * 4, 2 * time_dev
    row = lax.broadcasted_iota(jnp.int32, (rows, depth), 0)
    col = lax.broadcasted_iota(jnp.int32, (rows, depth), 1)
    q = row % 2
    s = (row // 2) % slots
    half = (row // (2 * slots)) % 2
    dest = row // (4 * slots)
    inner, place = dest // nz, dest % nz
    outer = jnp.where(place == 0, 0, jnp.where(place == 1, nz - 1, place - 1))
    m_index = (outer * INNER + inner) * slots + s
    order = jnp.zeros((rows, depth), jnp.int32)
    for m in range(m_total):
        order = jnp.where(m_index == m, az_ref[m], order)
    part = col // time_dev
    t = time_base + col % time_dev
    quarter = time_total // 4
    shift = jnp.where(q == part, 0, jnp.where(q == 0, -quarter, quarter))
    phase = (order * t + shift) & (time_total - 1)
    phase = jnp.where(phase > time_total // 2, phase - time_total, phase)
    sn = sin_half(phase.astype(jnp.float32) * (math.pi / time_total))
    value = (1.0 - 2.0 * sn * sn) * (1.0 / math.sqrt(time_total))
    upper = value.astype(jnp.bfloat16)
    lower = (value - upper.astype(jnp.float32)).astype(jnp.bfloat16)
    return jnp.where(half == 0, upper.astype(jnp.float32), lower.astype(jnp.float32)).astype(jnp.bfloat16)


def kernel(
    dims, az_hbm, live_hbm, vis_ref, proj_ref, kl_hbm, out_ref,
    vbuf, pbuf, az_ref, live_ref, kl_ref, table, sbuf, rbuf1, sbuf2, rbuf2, rlast, keep, pall, lhs, res,
    vsem, psem, csem, ysend, yrecv, zsend, zrecv, fsend, frecv, opened,
):
    nz, nf, units, slots, pols, bl, modes, chans, time_dev, time_total, m_total = dims
    tm, fi = lax.axis_index("tm"), lax.axis_index("freq")
    zi, yi = tm // INNER, tm % INNER
    partner = zi * INNER + (1 - yi)
    last = units - 1
    here_z = place_of(zi, nz)
    spans = (pl.ds(0, 1), pl.ds(1, 1), pl.ds(2, nz - 2))

    def z_peer(o):
        return lax.rem(zi + o, nz) * INNER + yi

    def f_peer(o):
        return lax.rem(fi + o, nf)

    def vis_copy(u):
        return pltpu.make_async_copy(vis_ref.at[:, pl.ds(u * CB, CB)], vbuf.at[u], vsem.at[u])

    def fetch(u):
        for part in range(2):
            for c in range(CB):
                pltpu.make_async_copy(vis_ref.at[part, u * CB + c], vbuf.at[u, part, c], vsem.at[u]).start()

    def remote(src, dst, send, recv, device):
        return pltpu.make_async_remote_copy(
            src_ref=src, dst_ref=dst, send_sem=send, recv_sem=recv, device_id=device, device_id_type=MESH
        )

    def y_copy(u, j):
        return remote(
            sbuf.at[u, 1 - yi, spans[j]], rbuf1.at[u, spans[j]], ysend.at[0], yrecv.at[j, u], (partner, fi)
        )

    def y_last():
        return remote(sbuf2.at[last, 0], rbuf1.at[last, 0], ysend.at[1], yrecv.at[0, last], (partner, fi))

    def z_copy(u, o):
        return remote(
            sbuf2.at[u, place_of(lax.rem(zi + o, nz), nz)], rbuf2.at[u, o - 1], zsend.at[0], zrecv.at[u], (z_peer(o), fi)
        )

    def z_last(o):
        return remote(
            sbuf.at[last, :, place_of(lax.rem(zi + o, nz), nz)], rlast.at[o - 1], zsend.at[1], zrecv.at[last], (z_peer(o), fi)
        )

    def f_copy(u, o):
        return remote(pall.at[fi, u], pall.at[fi, u], fsend.at[0], frecv.at[0], (tm, f_peer(o)))

    az_copy = pltpu.make_async_copy(az_hbm, az_ref, csem.at[0])
    live_copy = pltpu.make_async_copy(live_hbm, live_ref, csem.at[1])
    kl_copy = pltpu.make_async_copy(kl_hbm, kl_ref, csem.at[2])
    proj_copy = pltpu.make_async_copy(proj_ref, pbuf, psem.at[0])

    az_copy.start()
    for u in (0, last):
        fetch(u)
    barrier = pltpu.get_barrier_semaphore()
    pl.semaphore_signal(barrier, inc=1, device_id=(partner, fi), device_id_type=MESH)
    for o in range(1, nz):
        @pl.when((zi + o != nz) | (zi == 1))
        def _():
            pl.semaphore_signal(barrier, inc=1, device_id=(z_peer(o), fi), device_id_type=MESH)

    for o in range(1, nf):
        pl.semaphore_signal(barrier, inc=1, device_id=(tm, f_peer(o)), device_id_type=MESH)
    for u in range(1, last):
        fetch(u)
    live_copy.start()
    kl_copy.start()

    az_copy.wait()
    table[...] = build_tables(az_ref, m_total, nz, slots, time_dev, time_total, tm * time_dev)

    dests = nz * INNER
    rows = 4 * CB
    cols = pols * bl
    sub = lax.broadcasted_iota(jnp.int32, (dests, rows, cols), 1)

    def transform(u):
        vis_copy(u).wait()
        pair = []
        for c in range(CB):
            stream = jnp.concatenate([vbuf[u, 0, c], vbuf[u, 1, c]], axis=0)
            x = jnp.dot(table[...], stream, preferred_element_type=jnp.float32)
            x = x.reshape(dests, rows, cols)
            pair.append(x + pltpu.roll(x, 4, 1))
        block = jnp.where(sub < 4, pair[0], pair[1]).astype(jnp.bfloat16)
        sbuf[u] = block.reshape(INNER, nz, rows, cols)

    transform(0)
    pl.semaphore_wait(barrier, nf + 1 + (nz - 2) * jnp.minimum(zi, 1))

    @pl.when(zi == 1)
    def _():
        pl.semaphore_signal(opened, inc=1, device_id=(yi, fi), device_id_type=MESH)

    def parts_of(k, act):
        for j, delay in enumerate(DELAY):
            @pl.when(((k == 0) | (k > delay)) & (k < last + delay))
            def _():
                act(jnp.maximum(k - delay, 0), j)

    def send(u, j):
        y_copy(u, j).start()

    late = fi % 2

    @pl.when(late == 0)
    def _():
        parts_of(0, send)

    transform(last)
    for o in range(1, nz):
        @pl.when((zi > 0) | (o == 1))
        def _():
            z_last(o).start()

    def spread_units(u, carry):
        @pl.when(u < last)
        def _():
            transform(u)

        @pl.when(u >= late * 4)
        def _():
            parts_of(u - late * 4, send)

        return carry

    lax.fori_loop(1, last + max(DELAY) + 4, spread_units, 0)
    proj_copy.start()

    @pl.when(zi == 0)
    def _():
        pl.semaphore_wait(opened, 1)
        for o in range(2, nz):
            z_last(o).start()


    kl_copy.wait()
    live_copy.wait()
    width = chans * slots * 2
    spread_row = lax.broadcasted_iota(jnp.int32, (chans, width), 0)
    spread_col = lax.broadcasted_iota(jnp.int32, (chans, width), 1)
    spread = jnp.where(spread_col // (slots * 2) == spread_row, 1.0, 0.0).astype(jnp.bfloat16)
    lane = lax.broadcasted_iota(jnp.int32, (chans, width), 1) % (slots * 2)
    for s in range(slots):
        w_re = jnp.dot(kl_ref[s, 0], spread, preferred_element_type=jnp.float32)
        w_im = jnp.dot(kl_ref[s, 1], spread, preferred_element_type=jnp.float32)
        lhs[s, 0] = jnp.where(lane == 2 * s, w_re, jnp.where(lane == 2 * s + 1, -w_im, 0.0)).astype(jnp.bfloat16)
        lhs[s, 1] = jnp.where(lane == 2 * s, w_im, jnp.where(lane == 2 * s + 1, w_re, 0.0)).astype(jnp.bfloat16)

    prow = lax.broadcasted_iota(jnp.int32, (rows, 2 * modes), 0)
    plane = lax.broadcasted_iota(jnp.int32, (rows, 2 * modes), 1)

    def combine(u, j):
        y_copy(u, j).wait_recv()
        total = sbuf[u, yi, spans[j]].astype(jnp.float32) + rbuf1[u, spans[j]].astype(jnp.float32)
        sbuf2[u, spans[j]] = total.astype(jnp.bfloat16)
        for target in ((0,), (nz - 1,), range(1, nz - 1))[j]:
            @pl.when(zi != target)
            def _():
                z_copy(u, lax.rem(target + nz - zi, nz)).start()

    def combine_last():
        remote(rlast, rlast, zsend.at[1], zrecv.at[last], (partner, fi)).wait_recv()
        total = sbuf[last, :, here_z].astype(jnp.float32)
        for o in range(1, nz):
            total = total + rlast[o - 1].astype(jnp.float32)
        mine = yi == 0
        keep[...] = jnp.where(mine, total[0], total[1])
        sbuf2[last, 0] = jnp.where(mine, total[1], total[0]).astype(jnp.bfloat16)
        y_last().start()

    def project(u, total):
        vectors = jnp.concatenate([total[:, p * bl:(p + 1) * bl] for p in range(pols)], axis=0).astype(jnp.bfloat16)
        first = jnp.zeros((rows, 2 * modes), jnp.float32)
        second = first
        count = jnp.zeros((rows, 2 * modes), jnp.int32)
        for c in range(CB):
            for s in range(slots):
                part = lax.dot_general(
                    vectors, pbuf[s, u * CB + c], (((1,), (1,)), ((), ())), preferred_element_type=jnp.float32
                )
                here = prow // 2 == c * slots + s
                first = jnp.where(here, part[:rows, :2 * modes], first)
                second = jnp.where(here, part[rows:, 2 * modes:], second)
                live = [live_ref[s, p, u * CB + c] for p in range(pols)]
                count = jnp.where(here, jnp.where(plane < modes, live[0], live[1]), count)
        low = plane < modes
        direct = jnp.where(low, first, pltpu.roll(second, modes, 1))
        cross = jnp.where(low, pltpu.roll(first, modes, 1), second)
        real_row = prow % 2 == 0
        cross = jnp.where(real_row, -pltpu.roll(cross, rows - 1, 0), pltpu.roll(cross, 1, 0))
        kept = jnp.where(plane % modes < count, direct + cross, 0.0)
        pall[fi, u] = kept.astype(jnp.bfloat16)
        for o in range(1, nf):
            f_copy(u, o).start()

    def project_outer(u):
        remote(rbuf2.at[u], rbuf2.at[u], zsend.at[0], zrecv.at[u], (partner, fi)).wait_recv()
        total = sbuf2[u, here_z].astype(jnp.float32)
        for o in range(1, nz):
            total = total + rbuf2[u, o - 1].astype(jnp.float32)
        project(u, total)

    def project_last():
        y_last().wait_recv()
        project(last, keep[...] + rbuf1[last, 0].astype(jnp.float32))

    lags = [lag + delay for lag, delay in zip(LAG, DELAY)]
    lag = jnp.where(zi == 0, lags[0], jnp.where(zi == nz - 1, lags[1], lags[2]))

    def step(k, carry):
        parts_of(k, combine)

        @pl.when(k == 2)
        def _():
            proj_copy.wait()

        @pl.when(k == 4 + 1 * (1 - jnp.minimum(zi, 1)))
        def _():
            combine_last()

        @pl.when((k >= lag) & (k < last + lag))
        def _():
            project_outer(k - lag)

        @pl.when(k == last + 1)
        def _():
            project_last()

        return carry

    lax.fori_loop(0, last + max(lags), step, 0)

    everything = sbuf.at[pl.ds(0, last), 0]
    remote(everything, everything, ysend.at[0], yrecv.at[0, 0], (partner, fi)).wait_send()
    y_last().wait_send()
    everything = sbuf2.at[pl.ds(0, last), pl.ds(0, nz - 1)]
    remote(everything, everything, zsend.at[0], zrecv.at[0], (partner, fi)).wait_send()
    remote(rlast, rlast, zsend.at[1], zrecv.at[last], (partner, fi)).wait_send()
    everything = pall.at[pl.ds(0, nf - 1)]
    gather = remote(everything, everything, fsend.at[0], frecv.at[0], (partner, fi))
    gather.wait_send()
    gather.wait_recv()

    gathered = pall[...].reshape(nf * units * rows, 2 * modes)
    per = modes // nf
    for s in range(slots):
        for q in range(2):
            i = 2 * s + q
            res[i] = lax.dot_general(
                gathered, lhs[s, q], (((0,), (1,)), ((), ())), preferred_element_type=jnp.float32
            )
            for p in range(pols):
                at = pl.multiple_of(p * modes + fi * per, per)
                out_ref[s, q, p] = res[i, pl.ds(at, per), :]


def shards(visibilities, projection, kl_weight, azimuthal, live_mode_totals):
    nt, nf = lax.axis_size("tm"), lax.axis_size("freq")
    nz = nt // INNER
    time_dev, columns = visibilities.shape[2], visibilities.shape[3]
    slots, per_dev, pols, _, modes, bl = projection.shape
    chans = kl_weight.shape[3]
    units = per_dev // CB
    time_total = time_dev * nt
    m_total = azimuthal.shape[0]
    assert slots == 2 and pols == 2 and time_total & (time_total - 1) == 0 and units > max(DELAY) + 1 and nz > 2
    rows = 4 * CB
    dims = (nz, nf, units, slots, pols, bl, modes, chans, time_dev, time_total, m_total)
    bf16, f32 = jnp.bfloat16, jnp.float32
    flat = projection.reshape(slots, per_dev, pols * 2 * modes, bl)
    live = jnp.swapaxes(live_mode_totals, 1, 2)
    out = pl.pallas_call(
        functools.partial(kernel, dims),
        out_shape=pltpu.VMEM((slots, 2, pols, modes // nf, chans), f32),
        in_specs=[pl.BlockSpec(memory_space=pl.ANY)] * 5,
        out_specs=pl.BlockSpec(memory_space=pltpu.VMEM),
        scratch_shapes=[
            pltpu.VMEM((units, 2, CB, time_dev, columns), bf16),
            pltpu.VMEM(flat.shape, bf16),
            pltpu.SMEM(azimuthal.shape, jnp.int32),
            pltpu.SMEM(live.shape, jnp.int32),
            pltpu.VMEM(kl_weight.shape, bf16),
            pltpu.VMEM((nt * 8, 2 * time_dev), bf16),
            pltpu.VMEM((units, INNER, nz, rows, columns), bf16),
            pltpu.VMEM((units, nz, rows, columns), bf16),
            pltpu.VMEM((units, nz, rows, columns), bf16),
            pltpu.VMEM((units, nz - 1, rows, columns), bf16),
            pltpu.VMEM((nz - 1, INNER, rows, columns), bf16),
            pltpu.VMEM((rows, columns), f32),
            pltpu.VMEM((nf, units, rows, 2 * modes), bf16),
            pltpu.VMEM((slots, 2, chans, chans * slots * 2), bf16),
            pltpu.VMEM((slots * 2, pols * modes, chans), f32),
            pltpu.SemaphoreType.DMA((units,)),
            pltpu.SemaphoreType.DMA((1,)),
            pltpu.SemaphoreType.DMA((3,)),
            pltpu.SemaphoreType.DMA((2,)),
            pltpu.SemaphoreType.DMA((3, units)),
            pltpu.SemaphoreType.DMA((2,)),
            pltpu.SemaphoreType.DMA((units,)),
            pltpu.SemaphoreType.DMA((1,)),
            pltpu.SemaphoreType.DMA((1,)),
            pltpu.SemaphoreType.REGULAR,
        ],
        compiler_params=pltpu.CompilerParams(collective_id=0, has_side_effects=True),
    )(azimuthal, live, visibilities, flat, kl_weight)
    return jnp.transpose(out, (0, 1, 4, 2, 3))


def solution(mesh):
    return jax.shard_map(
        shards,
        mesh=mesh,
        in_specs=(
            P(None, "freq", "tm", None),
            P("tm", "freq", None, None, None, None),
            P("tm", None, None, None),
            P(),
            P("tm", "freq", None),
        ),
        out_specs=P("tm", None, None, None, "freq"),
        check_vma=False,
    )
```

```python
import functools
import math

import jax
import jax.numpy as jnp
from jax import lax
from jax.experimental import pallas as pl
from jax.experimental.pallas import tpu as pltpu
from jax.sharding import PartitionSpec as P

MESH = pl.DeviceIdType.MESH
INNER = 2
CB = 2
DELAY = (0, 1, 2)
LAG = (5, 4, 4)


def sin_half(x):
    y = x * x
    acc = jnp.full_like(x, -1.0 / math.factorial(15))
    for n in (13, 11, 9, 7, 5, 3, 1):
        sign = 1.0 if n % 4 == 1 else -1.0
        acc = acc * y + sign / math.factorial(n)
    return acc * x


def place_of(z, nz):
    return jnp.where(z == 0, 0, jnp.where(z == nz - 1, 1, z + 1))


def build_tables(az_ref, m_total, nz, slots, time_dev, time_total, time_base):
    rows, depth = nz * INNER * slots * 4, 2 * time_dev
    row = lax.broadcasted_iota(jnp.int32, (rows, depth), 0)
    col = lax.broadcasted_iota(jnp.int32, (rows, depth), 1)
    q = row % 2
    s = (row // 2) % slots
    half = (row // (2 * slots)) % 2
    dest = row // (4 * slots)
    inner, place = dest // nz, dest % nz
    outer = jnp.where(place == 0, 0, jnp.where(place == 1, nz - 1, place - 1))
    m_index = (outer * INNER + inner) * slots + s
    order = jnp.zeros((rows, depth), jnp.int32)
    for m in range(m_total):
        order = jnp.where(m_index == m, az_ref[m], order)
    part = col // time_dev
    t = time_base + col % time_dev
    quarter = time_total // 4
    shift = jnp.where(q == part, 0, jnp.where(q == 0, -quarter, quarter))
    phase = (order * t + shift) & (time_total - 1)
    phase = jnp.where(phase > time_total // 2, phase - time_total, phase)
    sn = sin_half(phase.astype(jnp.float32) * (math.pi / time_total))
    value = (1.0 - 2.0 * sn * sn) * (1.0 / math.sqrt(time_total))
    upper = value.astype(jnp.bfloat16)
    lower = (value - upper.astype(jnp.float32)).astype(jnp.bfloat16)
    return jnp.where(half == 0, upper.astype(jnp.float32), lower.astype(jnp.float32)).astype(jnp.bfloat16)


def kernel(
    dims, az_hbm, live_hbm, vis_ref, proj_ref, kl_hbm, out_ref,
    vbuf, pbuf, az_ref, live_ref, kl_ref, table, sbuf, rbuf1, sbuf2, rbuf2, rlast, keep, pall, lhs, res,
    vsem, psem, csem, ysend, yrecv, zsend, zrecv, fsend, frecv, opened,
):
    nz, nf, units, slots, pols, bl, modes, chans, time_dev, time_total, m_total = dims
    tm, fi = lax.axis_index("tm"), lax.axis_index("freq")
    zi, yi = tm // INNER, tm % INNER
    partner = zi * INNER + (1 - yi)
    last = units - 1
    here_z = place_of(zi, nz)
    spans = (pl.ds(0, 1), pl.ds(1, 1), pl.ds(2, nz - 2))

    def z_peer(o):
        return lax.rem(zi + o, nz) * INNER + yi

    def f_peer(o):
        return lax.rem(fi + o, nf)

    def vis_copy(u):
        return pltpu.make_async_copy(vis_ref.at[:, pl.ds(u * CB, CB)], vbuf.at[u], vsem.at[u])

    def fetch(u):
        for part in range(2):
            for c in range(CB):
                pltpu.make_async_copy(vis_ref.at[part, u * CB + c], vbuf.at[u, part, c], vsem.at[u]).start()

    def remote(src, dst, send, recv, device):
        return pltpu.make_async_remote_copy(
            src_ref=src, dst_ref=dst, send_sem=send, recv_sem=recv, device_id=device, device_id_type=MESH
        )

    def y_copy(u, j):
        return remote(
            sbuf.at[u, 1 - yi, spans[j]], rbuf1.at[u, spans[j]], ysend.at[0], yrecv.at[j, u], (partner, fi)
        )

    def y_last():
        return remote(sbuf2.at[last, 0], rbuf1.at[last, 0], ysend.at[1], yrecv.at[0, last], (partner, fi))

    def z_copy(u, o):
        return remote(
            sbuf2.at[u, place_of(lax.rem(zi + o, nz), nz)], rbuf2.at[u, o - 1], zsend.at[0], zrecv.at[u], (z_peer(o), fi)
        )

    def z_last(o):
        return remote(
            sbuf.at[last, :, place_of(lax.rem(zi + o, nz), nz)], rlast.at[o - 1], zsend.at[1], zrecv.at[last], (z_peer(o), fi)
        )

    def f_copy(u, o):
        return remote(pall.at[fi, u], pall.at[fi, u], fsend.at[0], frecv.at[0], (tm, f_peer(o)))

    az_copy = pltpu.make_async_copy(az_hbm, az_ref, csem.at[0])
    live_copy = pltpu.make_async_copy(live_hbm, live_ref, csem.at[1])
    kl_copy = pltpu.make_async_copy(kl_hbm, kl_ref, csem.at[2])
    proj_copy = pltpu.make_async_copy(proj_ref, pbuf, psem.at[0])

    az_copy.start()
    for u in (0, last):
        fetch(u)
    barrier = pltpu.get_barrier_semaphore()
    pl.semaphore_signal(barrier, inc=1, device_id=(partner, fi), device_id_type=MESH)
    for o in range(1, nz):
        @pl.when((zi + o != nz) | (zi == 1))
        def _():
            pl.semaphore_signal(barrier, inc=1, device_id=(z_peer(o), fi), device_id_type=MESH)

    for o in range(1, nf):
        pl.semaphore_signal(barrier, inc=1, device_id=(tm, f_peer(o)), device_id_type=MESH)
    for u in range(1, last):
        fetch(u)
    live_copy.start()
    kl_copy.start()

    az_copy.wait()
    table[...] = build_tables(az_ref, m_total, nz, slots, time_dev, time_total, tm * time_dev)

    dests = nz * INNER
    rows = 4 * CB
    cols = pols * bl
    sub = lax.broadcasted_iota(jnp.int32, (dests, rows, cols), 1)

    def transform(u):
        vis_copy(u).wait()
        pair = []
        for c in range(CB):
            stream = jnp.concatenate([vbuf[u, 0, c], vbuf[u, 1, c]], axis=0)
            x = jnp.dot(table[...], stream, preferred_element_type=jnp.float32)
            x = x.reshape(dests, rows, cols)
            pair.append(x + pltpu.roll(x, 4, 1))
        block = jnp.where(sub < 4, pair[0], pair[1]).astype(jnp.bfloat16)
        sbuf[u] = block.reshape(INNER, nz, rows, cols)

    transform(0)
    pl.semaphore_wait(barrier, nf + 1 + (nz - 2) * jnp.minimum(zi, 1))

    @pl.when(zi == 1)
    def _():
        pl.semaphore_signal(opened, inc=1, device_id=(yi, fi), device_id_type=MESH)

    def parts_of(k, act):
        for j, delay in enumerate(DELAY):
            @pl.when(((k == 0) | (k > delay)) & (k < last + delay))
            def _():
                act(jnp.maximum(k - delay, 0), j)

    def send(u, j):
        y_copy(u, j).start()

    late = fi % 2

    @pl.when(late == 0)
    def _():
        parts_of(0, send)

    transform(last)
    for o in range(1, nz):
        @pl.when((zi > 0) | (o == 1))
        def _():
            z_last(o).start()

    def spread_units(u, carry):
        @pl.when(u < last)
        def _():
            transform(u)

        @pl.when(u >= late * 4)
        def _():
            parts_of(u - late * 4, send)

        return carry

    lax.fori_loop(1, last + max(DELAY) + 4, spread_units, 0)
    proj_copy.start()

    @pl.when(zi == 0)
    def _():
        pl.semaphore_wait(opened, 1)
        for o in range(2, nz):
            z_last(o).start()


    kl_copy.wait()
    live_copy.wait()
    width = chans * slots * 2
    spread_row = lax.broadcasted_iota(jnp.int32, (chans, width), 0)
    spread_col = lax.broadcasted_iota(jnp.int32, (chans, width), 1)
    spread = jnp.where(spread_col // (slots * 2) == spread_row, 1.0, 0.0).astype(jnp.bfloat16)
    lane = lax.broadcasted_iota(jnp.int32, (chans, width), 1) % (slots * 2)
    for s in range(slots):
        w_re = jnp.dot(kl_ref[s, 0], spread, preferred_element_type=jnp.float32)
        w_im = jnp.dot(kl_ref[s, 1], spread, preferred_element_type=jnp.float32)
        lhs[s, 0] = jnp.where(lane == 2 * s, w_re, jnp.where(lane == 2 * s + 1, -w_im, 0.0)).astype(jnp.bfloat16)
        lhs[s, 1] = jnp.where(lane == 2 * s, w_im, jnp.where(lane == 2 * s + 1, w_re, 0.0)).astype(jnp.bfloat16)

    prow = lax.broadcasted_iota(jnp.int32, (rows, 2 * modes), 0)
    plane = lax.broadcasted_iota(jnp.int32, (rows, 2 * modes), 1)

    def combine(u, j):
        y_copy(u, j).wait_recv()
        total = sbuf[u, yi, spans[j]].astype(jnp.float32) + rbuf1[u, spans[j]].astype(jnp.float32)
        sbuf2[u, spans[j]] = total.astype(jnp.bfloat16)
        for target in ((0,), (nz - 1,), range(1, nz - 1))[j]:
            @pl.when(zi != target)
            def _():
                z_copy(u, lax.rem(target + nz - zi, nz)).start()

    def combine_last():
        remote(rlast, rlast, zsend.at[1], zrecv.at[last], (partner, fi)).wait_recv()
        total = sbuf[last, :, here_z].astype(jnp.float32)
        for o in range(1, nz):
            total = total + rlast[o - 1].astype(jnp.float32)
        mine = yi == 0
        keep[...] = jnp.where(mine, total[0], total[1])
        sbuf2[last, 0] = jnp.where(mine, total[1], total[0]).astype(jnp.bfloat16)
        y_last().start()

    def project(u, total):
        vectors = jnp.concatenate([total[:, p * bl:(p + 1) * bl] for p in range(pols)], axis=0).astype(jnp.bfloat16)
        first = jnp.zeros((rows, 2 * modes), jnp.float32)
        second = first
        count = jnp.zeros((rows, 2 * modes), jnp.int32)
        for c in range(CB):
            for s in range(slots):
                part = lax.dot_general(
                    vectors, pbuf[s, u * CB + c], (((1,), (1,)), ((), ())), preferred_element_type=jnp.float32
                )
                here = prow // 2 == c * slots + s
                first = jnp.where(here, part[:rows, :2 * modes], first)
                second = jnp.where(here, part[rows:, 2 * modes:], second)
                live = [live_ref[s, p, u * CB + c] for p in range(pols)]
                count = jnp.where(here, jnp.where(plane < modes, live[0], live[1]), count)
        low = plane < modes
        direct = jnp.where(low, first, pltpu.roll(second, modes, 1))
        cross = jnp.where(low, pltpu.roll(first, modes, 1), second)
        real_row = prow % 2 == 0
        cross = jnp.where(real_row, -pltpu.roll(cross, rows - 1, 0), pltpu.roll(cross, 1, 0))
        kept = jnp.where(plane % modes < count, direct + cross, 0.0)
        pall[fi, u] = kept.astype(jnp.bfloat16)
        for o in range(1, nf):
            f_copy(u, o).start()

    def project_outer(u):
        remote(rbuf2.at[u], rbuf2.at[u], zsend.at[0], zrecv.at[u], (partner, fi)).wait_recv()
        total = sbuf2[u, here_z].astype(jnp.float32)
        for o in range(1, nz):
            total = total + rbuf2[u, o - 1].astype(jnp.float32)
        project(u, total)

    def project_last():
        y_last().wait_recv()
        project(last, keep[...] + rbuf1[last, 0].astype(jnp.float32))

    lags = [lag + delay for lag, delay in zip(LAG, DELAY)]
    lag = jnp.where(zi == 0, lags[0], jnp.where(zi == nz - 1, lags[1], lags[2]))

    def step(k, carry):
        parts_of(k, combine)

        @pl.when(k == 2)
        def _():
            proj_copy.wait()

        @pl.when(k == 5 + 1 * (1 - jnp.minimum(zi, 1)))
        def _():
            combine_last()

        @pl.when((k >= lag) & (k < last + lag))
        def _():
            project_outer(k - lag)

        @pl.when(k == last + 1)
        def _():
            project_last()

        return carry

    lax.fori_loop(0, last + max(lags), step, 0)

    everything = sbuf.at[pl.ds(0, last), 0]
    remote(everything, everything, ysend.at[0], yrecv.at[0, 0], (partner, fi)).wait_send()
    y_last().wait_send()
    everything = sbuf2.at[pl.ds(0, last), pl.ds(0, nz - 1)]
    remote(everything, everything, zsend.at[0], zrecv.at[0], (partner, fi)).wait_send()
    remote(rlast, rlast, zsend.at[1], zrecv.at[last], (partner, fi)).wait_send()
    everything = pall.at[pl.ds(0, nf - 1)]
    gather = remote(everything, everything, fsend.at[0], frecv.at[0], (partner, fi))
    gather.wait_send()
    gather.wait_recv()

    gathered = pall[...].reshape(nf * units * rows, 2 * modes)
    per = modes // nf
    for s in range(slots):
        for q in range(2):
            i = 2 * s + q
            res[i] = lax.dot_general(
                gathered, lhs[s, q], (((0,), (1,)), ((), ())), preferred_element_type=jnp.float32
            )
            for p in range(pols):
                at = pl.multiple_of(p * modes + fi * per, per)
                out_ref[s, q, p] = res[i, pl.ds(at, per), :]


def shards(visibilities, projection, kl_weight, azimuthal, live_mode_totals):
    nt, nf = lax.axis_size("tm"), lax.axis_size("freq")
    nz = nt // INNER
    time_dev, columns = visibilities.shape[2], visibilities.shape[3]
    slots, per_dev, pols, _, modes, bl = projection.shape
    chans = kl_weight.shape[3]
    units = per_dev // CB
    time_total = time_dev * nt
    m_total = azimuthal.shape[0]
    assert slots == 2 and pols == 2 and time_total & (time_total - 1) == 0 and units > max(DELAY) + 1 and nz > 2
    rows = 4 * CB
    dims = (nz, nf, units, slots, pols, bl, modes, chans, time_dev, time_total, m_total)
    bf16, f32 = jnp.bfloat16, jnp.float32
    flat = projection.reshape(slots, per_dev, pols * 2 * modes, bl)
    live = jnp.swapaxes(live_mode_totals, 1, 2)
    out = pl.pallas_call(
        functools.partial(kernel, dims),
        out_shape=pltpu.VMEM((slots, 2, pols, modes // nf, chans), f32),
        in_specs=[pl.BlockSpec(memory_space=pl.ANY)] * 5,
        out_specs=pl.BlockSpec(memory_space=pltpu.VMEM),
        scratch_shapes=[
            pltpu.VMEM((units, 2, CB, time_dev, columns), bf16),
            pltpu.VMEM(flat.shape, bf16),
            pltpu.SMEM(azimuthal.shape, jnp.int32),
            pltpu.SMEM(live.shape, jnp.int32),
            pltpu.VMEM(kl_weight.shape, bf16),
            pltpu.VMEM((nt * 8, 2 * time_dev), bf16),
            pltpu.VMEM((units, INNER, nz, rows, columns), bf16),
            pltpu.VMEM((units, nz, rows, columns), bf16),
            pltpu.VMEM((units, nz, rows, columns), bf16),
            pltpu.VMEM((units, nz - 1, rows, columns), bf16),
            pltpu.VMEM((nz - 1, INNER, rows, columns), bf16),
            pltpu.VMEM((rows, columns), f32),
            pltpu.VMEM((nf, units, rows, 2 * modes), bf16),
            pltpu.VMEM((slots, 2, chans, chans * slots * 2), bf16),
            pltpu.VMEM((slots * 2, pols * modes, chans), f32),
            pltpu.SemaphoreType.DMA((units,)),
            pltpu.SemaphoreType.DMA((1,)),
            pltpu.SemaphoreType.DMA((3,)),
            pltpu.SemaphoreType.DMA((2,)),
            pltpu.SemaphoreType.DMA((3, units)),
            pltpu.SemaphoreType.DMA((2,)),
            pltpu.SemaphoreType.DMA((units,)),
            pltpu.SemaphoreType.DMA((1,)),
            pltpu.SemaphoreType.DMA((1,)),
            pltpu.SemaphoreType.REGULAR,
        ],
        compiler_params=pltpu.CompilerParams(collective_id=0, has_side_effects=True),
    )(azimuthal, live, visibilities, flat, kl_weight)
    return jnp.transpose(out, (0, 1, 4, 2, 3))


def solution(mesh):
    return jax.shard_map(
        shards,
        mesh=mesh,
        in_specs=(
            P(None, "freq", "tm", None),
            P("tm", "freq", None, None, None, None),
            P("tm", None, None, None),
            P(),
            P("tm", "freq", None),
        ),
        out_specs=P("tm", None, None, None, "freq"),
        check_vma=False,
    )
```

```python
import functools
import math

import jax
import jax.numpy as jnp
from jax import lax
from jax.experimental import pallas as pl
from jax.experimental.pallas import tpu as pltpu
from jax.sharding import PartitionSpec as P

MESH = pl.DeviceIdType.MESH
INNER = 2
CB = 2
DELAY = (0, 1, 2)
LAG = (5, 4, 4)


def sin_half(x):
    y = x * x
    acc = jnp.full_like(x, -1.0 / math.factorial(15))
    for n in (13, 11, 9, 7, 5, 3, 1):
        sign = 1.0 if n % 4 == 1 else -1.0
        acc = acc * y + sign / math.factorial(n)
    return acc * x


def place_of(z, nz):
    return jnp.where(z == 0, 0, jnp.where(z == nz - 1, 1, z + 1))


def build_tables(az_ref, m_total, nz, slots, time_dev, time_total, time_base):
    rows, depth = nz * INNER * slots * 4, 2 * time_dev
    row = lax.broadcasted_iota(jnp.int32, (rows, depth), 0)
    col = lax.broadcasted_iota(jnp.int32, (rows, depth), 1)
    q = row % 2
    s = (row // 2) % slots
    half = (row // (2 * slots)) % 2
    dest = row // (4 * slots)
    inner, place = dest // nz, dest % nz
    outer = jnp.where(place == 0, 0, jnp.where(place == 1, nz - 1, place - 1))
    m_index = (outer * INNER + inner) * slots + s
    order = jnp.zeros((rows, depth), jnp.int32)
    for m in range(m_total):
        order = jnp.where(m_index == m, az_ref[m], order)
    part = col // time_dev
    t = time_base + col % time_dev
    quarter = time_total // 4
    shift = jnp.where(q == part, 0, jnp.where(q == 0, -quarter, quarter))
    phase = (order * t + shift) & (time_total - 1)
    phase = jnp.where(phase > time_total // 2, phase - time_total, phase)
    sn = sin_half(phase.astype(jnp.float32) * (math.pi / time_total))
    value = (1.0 - 2.0 * sn * sn) * (1.0 / math.sqrt(time_total))
    upper = value.astype(jnp.bfloat16)
    lower = (value - upper.astype(jnp.float32)).astype(jnp.bfloat16)
    return jnp.where(half == 0, upper.astype(jnp.float32), lower.astype(jnp.float32)).astype(jnp.bfloat16)


def kernel(
    dims, az_hbm, live_hbm, vis_ref, proj_ref, kl_hbm, out_ref,
    vbuf, pbuf, az_ref, live_ref, kl_ref, table, sbuf, rbuf1, sbuf2, rbuf2, rlast, keep, pall, lhs, res,
    vsem, psem, csem, ysend, yrecv, zsend, zrecv, fsend, frecv, opened,
):
    nz, nf, units, slots, pols, bl, modes, chans, time_dev, time_total, m_total = dims
    tm, fi = lax.axis_index("tm"), lax.axis_index("freq")
    zi, yi = tm // INNER, tm % INNER
    partner = zi * INNER + (1 - yi)
    last = units - 1
    here_z = place_of(zi, nz)
    spans = (pl.ds(0, 1), pl.ds(1, 1), pl.ds(2, nz - 2))

    def z_peer(o):
        return lax.rem(zi + o, nz) * INNER + yi

    def f_peer(o):
        return lax.rem(fi + o, nf)

    def vis_copy(u):
        return pltpu.make_async_copy(vis_ref.at[:, pl.ds(u * CB, CB)], vbuf.at[u], vsem.at[u])

    def fetch(u):
        for c in range(CB):
            for part in range(2):
                arrived = vsem.at[u] if c == 0 else vsem.at[units]
                pltpu.make_async_copy(vis_ref.at[part, u * CB + c], vbuf.at[u, part, c], arrived).start()

    def remote(src, dst, send, recv, device):
        return pltpu.make_async_remote_copy(
            src_ref=src, dst_ref=dst, send_sem=send, recv_sem=recv, device_id=device, device_id_type=MESH
        )

    def y_copy(u, j):
        return remote(
            sbuf.at[u, 1 - yi, spans[j]], rbuf1.at[u, spans[j]], ysend.at[0], yrecv.at[j, u], (partner, fi)
        )

    def y_last():
        return remote(sbuf2.at[last, 0], rbuf1.at[last, 0], ysend.at[1], yrecv.at[0, last], (partner, fi))

    def z_copy(u, o):
        return remote(
            sbuf2.at[u, place_of(lax.rem(zi + o, nz), nz)], rbuf2.at[u, o - 1], zsend.at[0], zrecv.at[u], (z_peer(o), fi)
        )

    def z_last(o):
        return remote(
            sbuf.at[last, :, place_of(lax.rem(zi + o, nz), nz)], rlast.at[o - 1], zsend.at[1], zrecv.at[last], (z_peer(o), fi)
        )

    def f_copy(u, o):
        return remote(pall.at[fi, u], pall.at[fi, u], fsend.at[0], frecv.at[0], (tm, f_peer(o)))

    az_copy = pltpu.make_async_copy(az_hbm, az_ref, csem.at[0])
    live_copy = pltpu.make_async_copy(live_hbm, live_ref, csem.at[1])
    kl_copy = pltpu.make_async_copy(kl_hbm, kl_ref, csem.at[2])
    proj_copy = pltpu.make_async_copy(proj_ref, pbuf, psem.at[0])

    az_copy.start()
    fetch(0)
    vis_copy(last).start()
    barrier = pltpu.get_barrier_semaphore()
    pl.semaphore_signal(barrier, inc=1, device_id=(partner, fi), device_id_type=MESH)
    for o in range(1, nz):
        @pl.when((zi + o != nz) | (zi == 1))
        def _():
            pl.semaphore_signal(barrier, inc=1, device_id=(z_peer(o), fi), device_id_type=MESH)

    for o in range(1, nf):
        pl.semaphore_signal(barrier, inc=1, device_id=(tm, f_peer(o)), device_id_type=MESH)
    for u in range(1, last):
        vis_copy(u).start()
    live_copy.start()
    kl_copy.start()

    az_copy.wait()
    table[...] = build_tables(az_ref, m_total, nz, slots, time_dev, time_total, tm * time_dev)

    dests = nz * INNER
    rows = 4 * CB
    cols = pols * bl
    sub = lax.broadcasted_iota(jnp.int32, (dests, rows, cols), 1)

    def channel(u, c):
        stream = jnp.concatenate([vbuf[u, 0, c], vbuf[u, 1, c]], axis=0)
        x = jnp.dot(table[...], stream, preferred_element_type=jnp.float32).reshape(dests, rows, cols)
        return x + pltpu.roll(x, 4, 1)

    def store(u, pair):
        block = jnp.where(sub < 4, pair[0], pair[1]).astype(jnp.bfloat16)
        sbuf[u] = block.reshape(INNER, nz, rows, cols)

    def transform(u):
        vis_copy(u).wait()
        store(u, [channel(u, c) for c in range(CB)])

    def transform_first():
        pair = []
        for c in range(CB):
            ready = vsem.at[0 if c == 0 else units]
            pltpu.make_async_copy(vis_ref.at[:, c], vbuf.at[0, :, c], ready).wait()
            pair.append(channel(0, c))
        store(0, pair)

    transform_first()
    pl.semaphore_wait(barrier, nf + 1 + (nz - 2) * jnp.minimum(zi, 1))

    @pl.when(zi == 1)
    def _():
        pl.semaphore_signal(opened, inc=1, device_id=(yi, fi), device_id_type=MESH)

    def parts_of(k, act):
        for j, delay in enumerate(DELAY):
            @pl.when(((k == 0) | (k > delay)) & (k < last + delay))
            def _():
                act(jnp.maximum(k - delay, 0), j)

    def send(u, j):
        y_copy(u, j).start()

    late = fi % 2

    @pl.when(late == 0)
    def _():
        parts_of(0, send)

    transform(last)
    for o in range(1, nz):
        @pl.when((zi > 0) | (o == 1))
        def _():
            z_last(o).start()

    def spread_units(u, carry):
        @pl.when(u < last)
        def _():
            transform(u)

        @pl.when(u >= late * 4)
        def _():
            parts_of(u - late * 4, send)

        return carry

    lax.fori_loop(1, last + max(DELAY) + 4, spread_units, 0)
    proj_copy.start()

    @pl.when(zi == 0)
    def _():
        pl.semaphore_wait(opened, 1)
        for o in range(2, nz):
            z_last(o).start()


    kl_copy.wait()
    live_copy.wait()
    width = chans * slots * 2
    spread_row = lax.broadcasted_iota(jnp.int32, (chans, width), 0)
    spread_col = lax.broadcasted_iota(jnp.int32, (chans, width), 1)
    spread = jnp.where(spread_col // (slots * 2) == spread_row, 1.0, 0.0).astype(jnp.bfloat16)
    lane = lax.broadcasted_iota(jnp.int32, (chans, width), 1) % (slots * 2)
    for s in range(slots):
        w_re = jnp.dot(kl_ref[s, 0], spread, preferred_element_type=jnp.float32)
        w_im = jnp.dot(kl_ref[s, 1], spread, preferred_element_type=jnp.float32)
        lhs[s, 0] = jnp.where(lane == 2 * s, w_re, jnp.where(lane == 2 * s + 1, -w_im, 0.0)).astype(jnp.bfloat16)
        lhs[s, 1] = jnp.where(lane == 2 * s, w_im, jnp.where(lane == 2 * s + 1, w_re, 0.0)).astype(jnp.bfloat16)

    prow = lax.broadcasted_iota(jnp.int32, (rows, 2 * modes), 0)
    plane = lax.broadcasted_iota(jnp.int32, (rows, 2 * modes), 1)

    def combine(u, j):
        y_copy(u, j).wait_recv()
        total = sbuf[u, yi, spans[j]].astype(jnp.float32) + rbuf1[u, spans[j]].astype(jnp.float32)
        sbuf2[u, spans[j]] = total.astype(jnp.bfloat16)
        for target in ((0,), (nz - 1,), range(1, nz - 1))[j]:
            @pl.when(zi != target)
            def _():
                z_copy(u, lax.rem(target + nz - zi, nz)).start()

    def combine_last():
        remote(rlast, rlast, zsend.at[1], zrecv.at[last], (partner, fi)).wait_recv()
        total = sbuf[last, :, here_z].astype(jnp.float32)
        for o in range(1, nz):
            total = total + rlast[o - 1].astype(jnp.float32)
        mine = yi == 0
        keep[...] = jnp.where(mine, total[0], total[1])
        sbuf2[last, 0] = jnp.where(mine, total[1], total[0]).astype(jnp.bfloat16)
        y_last().start()

    def project(u, total):
        vectors = jnp.concatenate([total[:, p * bl:(p + 1) * bl] for p in range(pols)], axis=0).astype(jnp.bfloat16)
        first = jnp.zeros((rows, 2 * modes), jnp.float32)
        second = first
        count = jnp.zeros((rows, 2 * modes), jnp.int32)
        for c in range(CB):
            for s in range(slots):
                part = lax.dot_general(
                    vectors, pbuf[s, u * CB + c], (((1,), (1,)), ((), ())), preferred_element_type=jnp.float32
                )
                here = prow // 2 == c * slots + s
                first = jnp.where(here, part[:rows, :2 * modes], first)
                second = jnp.where(here, part[rows:, 2 * modes:], second)
                live = [live_ref[s, p, u * CB + c] for p in range(pols)]
                count = jnp.where(here, jnp.where(plane < modes, live[0], live[1]), count)
        low = plane < modes
        direct = jnp.where(low, first, pltpu.roll(second, modes, 1))
        cross = jnp.where(low, pltpu.roll(first, modes, 1), second)
        real_row = prow % 2 == 0
        cross = jnp.where(real_row, -pltpu.roll(cross, rows - 1, 0), pltpu.roll(cross, 1, 0))
        kept = jnp.where(plane % modes < count, direct + cross, 0.0)
        pall[fi, u] = kept.astype(jnp.bfloat16)
        for o in range(1, nf):
            f_copy(u, o).start()

    def project_outer(u):
        remote(rbuf2.at[u], rbuf2.at[u], zsend.at[0], zrecv.at[u], (partner, fi)).wait_recv()
        total = sbuf2[u, here_z].astype(jnp.float32)
        for o in range(1, nz):
            total = total + rbuf2[u, o - 1].astype(jnp.float32)
        project(u, total)

    def project_last():
        y_last().wait_recv()
        project(last, keep[...] + rbuf1[last, 0].astype(jnp.float32))

    lags = [lag + delay for lag, delay in zip(LAG, DELAY)]
    lag = jnp.where(zi == 0, lags[0], jnp.where(zi == nz - 1, lags[1], lags[2]))

    def step(k, carry):
        parts_of(k, combine)

        @pl.when(k == 2)
        def _():
            proj_copy.wait()

        @pl.when(k == 5 + 1 * (1 - jnp.minimum(zi, 1)))
        def _():
            combine_last()

        @pl.when((k >= lag) & (k < last + lag))
        def _():
            project_outer(k - lag)

        @pl.when(k == last + 1)
        def _():
            project_last()

        return carry

    lax.fori_loop(0, last + max(lags), step, 0)

    everything = sbuf.at[pl.ds(0, last), 0]
    remote(everything, everything, ysend.at[0], yrecv.at[0, 0], (partner, fi)).wait_send()
    y_last().wait_send()
    everything = sbuf2.at[pl.ds(0, last), pl.ds(0, nz - 1)]
    remote(everything, everything, zsend.at[0], zrecv.at[0], (partner, fi)).wait_send()
    remote(rlast, rlast, zsend.at[1], zrecv.at[last], (partner, fi)).wait_send()
    everything = pall.at[pl.ds(0, nf - 1)]
    gather = remote(everything, everything, fsend.at[0], frecv.at[0], (partner, fi))
    gather.wait_send()
    gather.wait_recv()

    gathered = pall[...].reshape(nf * units * rows, 2 * modes)
    per = modes // nf
    for s in range(slots):
        for q in range(2):
            i = 2 * s + q
            res[i] = lax.dot_general(
                gathered, lhs[s, q], (((0,), (1,)), ((), ())), preferred_element_type=jnp.float32
            )
            for p in range(pols):
                at = pl.multiple_of(p * modes + fi * per, per)
                out_ref[s, q, p] = res[i, pl.ds(at, per), :]


def shards(visibilities, projection, kl_weight, azimuthal, live_mode_totals):
    nt, nf = lax.axis_size("tm"), lax.axis_size("freq")
    nz = nt // INNER
    time_dev, columns = visibilities.shape[2], visibilities.shape[3]
    slots, per_dev, pols, _, modes, bl = projection.shape
    chans = kl_weight.shape[3]
    units = per_dev // CB
    time_total = time_dev * nt
    m_total = azimuthal.shape[0]
    assert slots == 2 and pols == 2 and time_total & (time_total - 1) == 0 and units > max(DELAY) + 1 and nz > 2
    rows = 4 * CB
    dims = (nz, nf, units, slots, pols, bl, modes, chans, time_dev, time_total, m_total)
    bf16, f32 = jnp.bfloat16, jnp.float32
    flat = projection.reshape(slots, per_dev, pols * 2 * modes, bl)
    live = jnp.swapaxes(live_mode_totals, 1, 2)
    out = pl.pallas_call(
        functools.partial(kernel, dims),
        out_shape=pltpu.VMEM((slots, 2, pols, modes // nf, chans), f32),
        in_specs=[pl.BlockSpec(memory_space=pl.ANY)] * 5,
        out_specs=pl.BlockSpec(memory_space=pltpu.VMEM),
        scratch_shapes=[
            pltpu.VMEM((units, 2, CB, time_dev, columns), bf16),
            pltpu.VMEM(flat.shape, bf16),
            pltpu.SMEM(azimuthal.shape, jnp.int32),
            pltpu.SMEM(live.shape, jnp.int32),
            pltpu.VMEM(kl_weight.shape, bf16),
            pltpu.VMEM((nt * 8, 2 * time_dev), bf16),
            pltpu.VMEM((units, INNER, nz, rows, columns), bf16),
            pltpu.VMEM((units, nz, rows, columns), bf16),
            pltpu.VMEM((units, nz, rows, columns), bf16),
            pltpu.VMEM((units, nz - 1, rows, columns), bf16),
            pltpu.VMEM((nz - 1, INNER, rows, columns), bf16),
            pltpu.VMEM((rows, columns), f32),
            pltpu.VMEM((nf, units, rows, 2 * modes), bf16),
            pltpu.VMEM((slots, 2, chans, chans * slots * 2), bf16),
            pltpu.VMEM((slots * 2, pols * modes, chans), f32),
            pltpu.SemaphoreType.DMA((units + 1,)),
            pltpu.SemaphoreType.DMA((1,)),
            pltpu.SemaphoreType.DMA((3,)),
            pltpu.SemaphoreType.DMA((2,)),
            pltpu.SemaphoreType.DMA((3, units)),
            pltpu.SemaphoreType.DMA((2,)),
            pltpu.SemaphoreType.DMA((units,)),
            pltpu.SemaphoreType.DMA((1,)),
            pltpu.SemaphoreType.DMA((1,)),
            pltpu.SemaphoreType.REGULAR,
        ],
        compiler_params=pltpu.CompilerParams(collective_id=0, has_side_effects=True),
    )(azimuthal, live, visibilities, flat, kl_weight)
    return jnp.transpose(out, (0, 1, 4, 2, 3))


def solution(mesh):
    return jax.shard_map(
        shards,
        mesh=mesh,
        in_specs=(
            P(None, "freq", "tm", None),
            P("tm", "freq", None, None, None, None),
            P("tm", None, None, None),
            P(),
            P("tm", "freq", None),
        ),
        out_specs=P("tm", None, None, None, "freq"),
        check_vma=False,
    )
```
